32 devices in a mesh: lat: 4 (over y, x), lon: 8 (over z, core).
Axes of the slice: x: 2, y: 2, z: 4, core: 2. Of those that a mesh axis runs over, the one named last changes fastest.
Arguments:
- input_field: bfloat16 [512, 512, 128], P('lat', 'lon'), may hold values from -6 to 6
- conv_one: bfloat16 [3, 3, 128, 128], replicated, may hold values from -0.1875 to 0.1875
- conv_two: bfloat16 [3, 3, 128, 128], replicated, may hold values from -0.1875 to 0.1875
- merge_weight: bfloat16 [512, 512], replicated, may hold values from -0.25 to 0.25
- norm_gains: float32 [4, 512], replicated, may hold values from 0.1 to 1.9
- attention_in: bfloat16 [512, 1536], replicated, may hold values from -0.25 to 0.25
- attention_out: bfloat16 [512, 512], replicated, may hold values from -0.25 to 0.25
- dense_in: bfloat16 [512, 2048], replicated, may hold values from -0.25 to 0.25
- dense_out: bfloat16 [2048, 512], replicated, may hold values from -0.125 to 0.125
- expand_weight: bfloat16 [512, 512], replicated, may hold values from -0.25 to 0.25
Outputs:
- output_field: bfloat16 [512, 512, 128], P('lat', 'lon')
The draws below stay inside these ranges and needn't reach their ends.
All inputs are finite; a program needn't handle non-finite values.
Results may differ from the reference program's by a relative error of at most 0.0095.
Values may be sent and summed in bfloat16 or wider, within the bound.
A program may use at most 128 MiB of HBM per device.

```python
import jax
import jax.numpy as jnp
from jax import lax

CHANNELS = 128
LATENT = 512
NUM_HEADS = 16
MLP_WIDTH = 2048
WINDOW = 16
HEAD_WIDTH = 32
LAT_CELLS = 512
LON_CELLS = 512


def level_of(stream_key, dims, shards, smallest, largest):
    factor_of = 1.0
    for axis_at, blocks in shards:
        draws = jax.random.uniform(jax.random.fold_in(jax.random.fold_in(stream_key, 6), axis_at), (blocks,), jnp.float32, smallest / len(shards), largest / len(shards))
        factor_of = factor_of * jnp.repeat(jnp.exp(draws), dims[axis_at] // blocks).reshape((-1,) + (1,) * (len(dims) - 1 - axis_at))
    return factor_of


def gaussian(own_key, extent, scale, bound, shards=(), kind=jnp.bfloat16):
    entries = scale * jax.random.normal(own_key, extent, jnp.float32)
    if shards:
        entries = entries * level_of(own_key, extent, shards, -0.22, 0.18)
    return jnp.clip(entries, -bound, bound).astype(kind)


def setup_inputs(seed: int = 0) -> dict:
    keys = jax.random.split(jax.random.key(seed), 11)
    return {
        "input_field": gaussian(keys[0], (LAT_CELLS, LON_CELLS, CHANNELS), 1.0, 6.0, ((0, 4), (1, 8))),
        "conv_one": gaussian(keys[1], (3, 3, CHANNELS, CHANNELS), (9 * CHANNELS) ** -0.5, 0.1875),
        "conv_two": gaussian(keys[2], (3, 3, CHANNELS, CHANNELS), (9 * CHANNELS) ** -0.5, 0.1875),
        "merge_weight": gaussian(keys[3], (4 * CHANNELS, LATENT), (4 * CHANNELS) ** -0.5, 0.25),
        "norm_gains": jnp.clip(1.0 + 0.18 * jax.random.normal(keys[4], (4, LATENT), jnp.float32), 0.1, 1.9),
        "attention_in": gaussian(keys[5], (LATENT, 3 * LATENT), LATENT ** -0.5, 0.25),
        "attention_out": gaussian(keys[6], (LATENT, LATENT), LATENT ** -0.5, 0.25),
        "dense_in": gaussian(keys[7], (LATENT, MLP_WIDTH), LATENT ** -0.5, 0.25),
        "dense_out": gaussian(keys[8], (MLP_WIDTH, LATENT), MLP_WIDTH ** -0.5, 0.125),
        "expand_weight": gaussian(keys[9], (LATENT, 4 * CHANNELS), LATENT ** -0.5, 0.25),
    }


EPSILON = 1e-06
FLOOR = 0.75

def conv_gelu(source, kernel, padding):
    result = lax.conv_general_dilated(source[None], kernel, (1, 1), padding, dimension_numbers=('NHWC', 'HWIO', 'NHWC'), preferred_element_type=jnp.float32)[0]
    return jax.nn.gelu(result)

def layer_norm(stream, gain):
    center = stream - lax.optimization_barrier(jnp.mean(stream, axis=-1, keepdims=True))
    spread = lax.optimization_barrier(jnp.mean(center * center, axis=-1, keepdims=True))
    return center * lax.rsqrt(spread + EPSILON) * gain

def head_norm(stream, gain):
    square = lax.optimization_barrier(jnp.mean(stream * stream, axis=-1, keepdims=True))
    return stream * gain / jnp.sqrt(jnp.maximum(square, FLOOR))

def project_heads(tokens, norm_gains, attention_in):
    count = tokens.shape[0]
    normed = layer_norm(tokens.astype(jnp.float32), norm_gains[0]).astype(jnp.bfloat16)
    projected = jnp.dot(normed, attention_in, preferred_element_type=jnp.float32)
    split_shape = (count, NUM_HEADS, HEAD_WIDTH)
    queries = head_norm(projected[:, :LATENT].reshape(split_shape), norm_gains[1].reshape(NUM_HEADS, HEAD_WIDTH)).astype(jnp.bfloat16)
    key_rows = head_norm(projected[:, LATENT:2 * LATENT].reshape(split_shape), norm_gains[2].reshape(NUM_HEADS, HEAD_WIDTH)).astype(jnp.bfloat16)
    values = projected[:, 2 * LATENT:].reshape(split_shape).astype(jnp.bfloat16)
    return (queries, key_rows, values)

def attend_window(queries, key_rows, values):
    scores = jnp.einsum('qhd,khd->hqk', queries.astype(jnp.float32), key_rows.astype(jnp.float32)) * HEAD_WIDTH ** (-0.5)
    expon = jnp.exp(scores)
    weights = (expon / lax.optimization_barrier(jnp.sum(expon, axis=-1, keepdims=True))).astype(jnp.bfloat16)
    gathered = jnp.einsum('hqk,khd->qhd', weights.astype(jnp.float32), values.astype(jnp.float32))
    return gathered.reshape(queries.shape[0], LATENT).astype(jnp.bfloat16)

def finish(tokens, attended, norm_gains, attention_out, dense_in, dense_out):
    mixed_tokens = (tokens.astype(jnp.float32) + jnp.dot(attended, attention_out, preferred_element_type=jnp.float32)).astype(jnp.bfloat16)
    normed_two = layer_norm(mixed_tokens.astype(jnp.float32), norm_gains[3]).astype(jnp.bfloat16)
    inner_units = jax.nn.gelu(jnp.dot(normed_two, dense_in, preferred_element_type=jnp.float32)).astype(jnp.bfloat16)
    return (mixed_tokens.astype(jnp.float32) + jnp.dot(inner_units, dense_out, preferred_element_type=jnp.float32)).astype(jnp.bfloat16)

def reference(input_field, conv_one, conv_two, merge_weight, norm_gains, attention_in, attention_out, dense_in, dense_out, expand_weight):
    first = conv_gelu(input_field, conv_one, 'SAME').astype(jnp.bfloat16)
    second = conv_gelu(first, conv_two, 'SAME').astype(jnp.bfloat16)
    half_lat = LAT_CELLS // 2
    half_lon = LON_CELLS // 2
    offset_lat = half_lat // WINDOW
    offset_lon = half_lon // WINDOW
    patches = second.reshape(half_lat, 2, half_lon, 2, CHANNELS).transpose(0, 2, 1, 3, 4).reshape(half_lat * half_lon, 4 * CHANNELS)
    coarse = jnp.dot(patches, merge_weight, preferred_element_type=jnp.float32).astype(jnp.bfloat16)
    grouped = coarse.reshape(WINDOW, offset_lat, WINDOW, offset_lon, LATENT).transpose(1, 3, 0, 2, 4).reshape(offset_lat * offset_lon, WINDOW * WINDOW, LATENT)

    def one_window(tokens):
        queries, key_rows, values = project_heads(tokens, norm_gains, attention_in)
        attended = attend_window(queries, key_rows, values)
        return finish(tokens, attended, norm_gains, attention_out, dense_in, dense_out)
    updated = lax.map(one_window, grouped)
    placed = updated.reshape(offset_lat, offset_lon, WINDOW, WINDOW, LATENT).transpose(2, 0, 3, 1, 4).reshape(half_lat * half_lon, LATENT)
    expanded = jnp.dot(placed, expand_weight, preferred_element_type=jnp.float32)
    expanded = expanded.reshape(half_lat, half_lon, 2, 2, CHANNELS).transpose(0, 2, 1, 3, 4).reshape(LAT_CELLS, LON_CELLS, CHANNELS)
    return (expanded + input_field.astype(jnp.float32)).astype(jnp.bfloat16)
```

```python
import functools
import math

import jax
import jax.numpy as jnp
from jax import lax
from jax.experimental import pallas as pl
from jax.experimental.pallas import tpu as pltpu
from jax.sharding import PartitionSpec as P

WINDOW = 16
HEAD_WIDTH = 32
EPSILON = 1e-06
FLOOR = 0.75
CHUNKS = 4
F32 = jnp.float32
BF16 = jnp.bfloat16
LIMIT = 56 * 1024 * 1024


def dot(a, b):
    return jnp.dot(a, b, preferred_element_type=F32)


def padded(cells, sides, width):
    for axis, dim in sides:
        count = lax.axis_size(axis)
        ends = count - 1
        head = lax.slice_in_dim(cells, 0, width, axis=dim)
        tail = lax.slice_in_dim(cells, cells.shape[dim] - width, cells.shape[dim], axis=dim)
        cells = jnp.concatenate(
            [
                lax.ppermute(tail, axis, [(i, (i + 1) % count) for i in range(ends)]),
                cells,
                lax.ppermute(head, axis, [((i + 1) % count, i) for i in range(ends)]),
            ],
            axis=dim,
        )
    return cells


def pair_kernel(kernel):
    taps, _, c, o = kernel.shape
    zero = jnp.zeros((taps, 1, c, o), kernel.dtype)
    left = jnp.concatenate([kernel, zero], axis=1).reshape(taps, 4 * c, o)
    right = jnp.concatenate([zero, kernel], axis=1).reshape(taps, 4 * c, o)
    return jnp.concatenate([left, right], axis=2).reshape(taps * 4 * c, 2 * o)


def encode_body(geo, place_ref, x_ref, w1_ref, w2_ref, mw_ref, out_ref, xs, fs, cs):
    (chunk, chunks, per_lat, per_lon, offset_lat, offset_lon, lat_total, lon_total, breadth, pairs) = geo
    band = pl.program_id(0)
    rows = 2 * offset_lat // chunks
    c = x_ref.shape[2]
    half = breadth // 2
    wide = breadth + 4

    @pl.when(band == 0)
    def _():
        xs[:, wide:, :] = jnp.zeros((rows + 4, xs.shape[1] - wide, c), F32)

    xs[:, :wide, :] = x_ref[...].astype(F32)
    quad = [
        xs[:, pl.ds(j, pairs, stride=2), :].astype(BF16) for j in range(4)
    ]
    lhs = jnp.concatenate(
        [q[a : a + rows + 2].reshape((rows + 2) * pairs, c) for a in range(3) for q in quad], axis=1
    )
    first = jax.nn.gelu(dot(lhs, w1_ref[...])).reshape(rows + 2, pairs, 2 * c)
    row = lax.broadcasted_iota(jnp.int32, first.shape, 0)
    pair = lax.broadcasted_iota(jnp.int32, first.shape, 1)
    lane = lax.broadcasted_iota(jnp.int32, first.shape, 2)
    lat_place = row + (place_ref[0] + band * 2 * offset_lat + chunk * rows - 1)
    lon_place = 2 * pair + (lane >= c).astype(jnp.int32) + (place_ref[1] - 1)
    inside = (lat_place >= 0) & (lat_place < lat_total) & (lon_place >= 0) & (lon_place < lon_total)
    fs[...] = jnp.where(inside, first, 0.0)
    near = fs[:, 0:half, :].astype(BF16)
    far = fs[:, pl.ds(1, half), :].astype(BF16)
    lhs = jnp.concatenate(
        [q[a : a + rows].reshape(rows * half, 2 * c) for a in range(3) for q in (near, far)], axis=1
    )
    second = jax.nn.gelu(dot(lhs, w2_ref[...])).astype(BF16)
    second = second.reshape(rows // 2, 2, half, 2 * c)
    patches = jnp.concatenate(
        [second[:, d].reshape(rows // 2 * half, 2 * c) for d in range(2)], axis=1
    )
    coarse = dot(patches, mw_ref[...]).astype(BF16).reshape(rows // 2, half, 4 * c)
    for u in range(rows // 2):
        cs[u, pl.ds(pl.multiple_of(band * half, half), half), :] = coarse[u]

    @pl.when(band == per_lat - 1)
    def _():
        count = per_lat * half
        tokens = per_lat * per_lon
        to = lax.broadcasted_iota(jnp.int32, (count, count), 0)
        of = lax.broadcasted_iota(jnp.int32, (count, count), 1)
        source = (to % tokens) * offset_lon + to // tokens
        move = (of == source).astype(F32).astype(BF16)
        for u in range(rows // 2):
            out_ref[u * count : (u + 1) * count, :] = dot(move, cs[u]).astype(BF16)


def encode(geo, place, widened, w1, w2, merge_weight):
    (chunk, chunks, per_lat, per_lon, offset_lat, offset_lon, lat_total, lon_total, breadth, pairs) = geo
    rows = 2 * offset_lat // chunks
    c = widened.shape[2]
    half = breadth // 2
    count = rows // 2 * per_lat * half
    full = lambda a: pl.BlockSpec(a.shape, lambda p: (0,) * a.ndim)
    flops = 2 * per_lat * ((rows + 2) * pairs + rows * half) * 12 * c * 2 * c
    return pl.pallas_call(
        functools.partial(encode_body, geo),
        grid=(per_lat,),
        in_specs=[
            pl.BlockSpec(memory_space=pltpu.SMEM),
            pl.BlockSpec(
                (pl.Element(rows + 4), pl.Element(breadth + 4), pl.Element(c)),
                lambda p: (p * 2 * offset_lat + chunk * rows, 0, 0),
            ),
            full(w1),
            full(w2),
            full(merge_weight),
        ],
        out_specs=pl.BlockSpec((count, 4 * c), lambda p: (0, 0)),
        out_shape=jax.ShapeDtypeStruct((count, 4 * c), BF16),
        scratch_shapes=[
            pltpu.VMEM((rows + 4, max(2 * pairs + 8, breadth + 8), c), F32),
            pltpu.VMEM((rows + 2, pairs, 2 * c), F32),
            pltpu.VMEM((rows // 2, per_lat * half, 4 * c), BF16),
        ],
        compiler_params=pltpu.CompilerParams(
            dimension_semantics=("arbitrary",), vmem_limit_bytes=LIMIT
        ),
        cost_estimate=pl.CostEstimate(flops=flops, bytes_accessed=4_000_000, transcendentals=0),
        name="encode",
    )(place, widened, w1, w2, merge_weight)


def layer_norm(stream, gain):
    center = stream - jnp.mean(stream, axis=-1, keepdims=True)
    spread = jnp.mean(center * center, axis=-1, keepdims=True)
    return center * lax.rsqrt(spread + EPSILON) * gain


def window_body(geo, x_ref, g_ref, ai_ref, ao_ref, di_ref, do_ref, out_ref):
    devices, windows, tokens = geo
    count, latent = x_ref.shape
    size = devices * tokens
    to = lax.broadcasted_iota(jnp.int32, (count, count), 0)
    of = lax.broadcasted_iota(jnp.int32, (count, count), 1)

    def sorted_row(i):
        return (i // tokens % windows) * size + i // (tokens * windows) * tokens + i % tokens

    gather = (to == sorted_row(of)).astype(F32).astype(BF16)
    scatter = (of == sorted_row(to)).astype(F32).astype(BF16)
    coarse = dot(gather, x_ref[...])
    gains = g_ref[...]
    normed = layer_norm(coarse, gains[0:1]).astype(BF16)
    head_row = lax.broadcasted_iota(jnp.int32, (latent, latent), 0) // HEAD_WIDTH
    head_col = lax.broadcasted_iota(jnp.int32, (latent, latent), 1) // HEAD_WIDTH
    spread = jnp.where(head_row == head_col, 1.0 / HEAD_WIDTH, 0.0).astype(BF16)

    def head_norm(stream, gain):
        square = dot((stream * stream).astype(BF16), spread)
        return (stream * gain * lax.rsqrt(jnp.maximum(square, FLOOR))).astype(BF16)

    queries = head_norm(dot(normed, ai_ref[:, :latent]), gains[1:2])
    key_rows = head_norm(dot(normed, ai_ref[:, latent : 2 * latent]), gains[2:3])
    values = dot(normed, ai_ref[:, 2 * latent :]).astype(BF16)
    group = 128
    heads = group // HEAD_WIDTH
    lane = lax.broadcasted_iota(jnp.int32, (size, group), 1) // HEAD_WIDTH
    marks = [(lane == h).astype(F32).astype(BF16) for h in range(heads)]
    scale = HEAD_WIDTH ** (-0.5) * math.log2(math.e)
    parts = []
    for win in range(windows):
        span = slice(win * size, (win + 1) * size)
        row_parts = []
        for at in range(0, latent, group):
            q = queries[span, at : at + group]
            k = key_rows[span, at : at + group]
            v = values[span, at : at + group]
            expons = []
            stacked = []
            for h in range(heads):
                scores = lax.dot_general(
                    q * marks[h], k, (((1,), (1,)), ((), ())), preferred_element_type=F32
                )
                expons.append(jnp.exp2(scores * scale).astype(BF16))
                stacked.append(jnp.concatenate([v * marks[h], marks[h]], axis=1))
            both = dot(jnp.concatenate(expons, axis=1), jnp.concatenate(stacked, axis=0))
            row_parts.append((both[:, :group] / both[:, group:]).astype(BF16))
        parts.append(jnp.concatenate(row_parts, axis=1))
    attended = jnp.concatenate(parts, axis=0)
    mixed = (coarse + dot(attended, ao_ref[...])).astype(BF16)
    normed_two = layer_norm(mixed.astype(F32), gains[3:4]).astype(BF16)
    total = mixed.astype(F32)
    width = di_ref.shape[1]
    step = min(512, width)
    for at in range(0, width, step):
        inner = jax.nn.gelu(dot(normed_two, di_ref[:, at : at + step])).astype(BF16)
        total = total + dot(inner, do_ref[at : at + step, :])
    out_ref[...] = dot(scatter, total.astype(BF16)).astype(BF16)


def windows_of(geo, tokens, gains, attention_in, attention_out, dense_in, dense_out):
    count, latent = tokens.shape
    flops = 2 * count * latent * (4 * latent + 2 * dense_in.shape[1] + 4 * count)
    return pl.pallas_call(
        functools.partial(window_body, geo),
        out_shape=jax.ShapeDtypeStruct(tokens.shape, BF16),
        in_specs=[pl.BlockSpec(memory_space=pltpu.VMEM)] * 6,
        out_specs=pl.BlockSpec(memory_space=pltpu.VMEM),
        compiler_params=pltpu.CompilerParams(vmem_limit_bytes=LIMIT),
        cost_estimate=pl.CostEstimate(flops=flops, bytes_accessed=8_000_000, transcendentals=0),
        name="windows",
    )(tokens, gains, attention_in, attention_out, dense_in, dense_out)


def expand_body(geo, aliased, ret_ref, x_ref, ew_ref, *rest):
    (chunk, chunks, per_lat, per_lon, offset_lat, offset_lon, breadth) = geo
    out_ref, os = rest[-2:]
    band = pl.program_id(0)
    lines = offset_lat // chunks
    c = x_ref.shape[2]
    half = breadth // 2
    tokens = per_lat * per_lon
    count = per_lat * half
    to = lax.broadcasted_iota(jnp.int32, (half, count), 0)
    of = lax.broadcasted_iota(jnp.int32, (half, count), 1)
    source = (to % offset_lon) * tokens + band * per_lon + to // offset_lon
    move = (of == source).astype(F32).astype(BF16)
    cells = jnp.concatenate(
        [dot(move, ret_ref[u * count : (u + 1) * count, :]).astype(BF16) for u in range(lines)], axis=0
    )
    made = dot(cells, ew_ref[...])
    for u in range(lines):
        for d in range(4):
            os[2 * u + d // 2, pl.ds(d % 2, half, stride=2), :] = made[
                u * half : (u + 1) * half, d * c : (d + 1) * c
            ]
    out_ref[...] = (os[...] + x_ref[...].astype(F32)).astype(BF16)


def expand(geo, returned, field, expand_weight, buffer):
    (chunk, chunks, per_lat, per_lon, offset_lat, offset_lon, breadth) = geo
    rows = 2 * offset_lat // chunks
    c = field.shape[2]
    aliased = buffer is not None
    place = pl.BlockSpec((rows, breadth, c), lambda p: (p * chunks + chunk, 0, 0))
    in_specs = [
        pl.BlockSpec(returned.shape, lambda p: (0, 0)),
        place,
        pl.BlockSpec(expand_weight.shape, lambda p: (0, 0)),
    ]
    args = [returned, field, expand_weight]
    if aliased:
        in_specs.append(pl.BlockSpec(memory_space=pl.ANY))
        args.append(buffer)
    return pl.pallas_call(
        functools.partial(expand_body, geo, aliased),
        grid=(per_lat,),
        in_specs=in_specs,
        out_specs=place,
        out_shape=jax.ShapeDtypeStruct(field.shape, BF16),
        scratch_shapes=[pltpu.VMEM((rows, breadth, c), F32)],
        input_output_aliases={3: 0} if aliased else {},
        compiler_params=pltpu.CompilerParams(
            dimension_semantics=("arbitrary",), vmem_limit_bytes=LIMIT
        ),
        cost_estimate=pl.CostEstimate(
            flops=2 * returned.size * 4 * c, bytes_accessed=3_000_000, transcendentals=0
        ),
        name="expand",
    )(*args)


def per_device(
    input_field,
    conv_one,
    conv_two,
    merge_weight,
    norm_gains,
    attention_in,
    attention_out,
    dense_in,
    dense_out,
    expand_weight,
):
    height, breadth, _ = input_field.shape
    latent = merge_weight.shape[1]
    lat_count = lax.axis_size("lat")
    lon_count = lax.axis_size("lon")
    per_lat = WINDOW // lat_count
    per_lon = WINDOW // lon_count
    offset_lat = height // (2 * per_lat)
    offset_lon = breadth // (2 * per_lon)
    tokens = per_lat * per_lon
    devices = lat_count * lon_count
    windows = offset_lat * offset_lon // devices // CHUNKS
    pairs = -(-(breadth // 2 + 1) // 16) * 16
    w1 = pair_kernel(conv_one)
    w2 = pair_kernel(conv_two)
    place = jnp.stack([lax.axis_index("lat") * height, lax.axis_index("lon") * breadth]).astype(jnp.int32)
    widened = padded(input_field, (("lat", 0), ("lon", 1)), 2)

    def exchange(cells):
        moved = lax.all_to_all(
            cells.reshape(devices, windows * tokens, latent),
            ("lat", "lon"),
            split_axis=0,
            concat_axis=0,
            tiled=True,
        )
        return moved.reshape(cells.shape)

    shape = (per_lat, per_lon, offset_lat, offset_lon)
    sent = [
        exchange(
            encode(
                (chunk, CHUNKS) + shape + (height * lat_count, breadth * lon_count, breadth, pairs),
                place,
                widened,
                w1,
                w2,
                merge_weight,
            )
        )
        for chunk in range(CHUNKS)
    ]
    returned = [
        exchange(
            windows_of(
                (devices, windows, tokens), cells, norm_gains, attention_in, attention_out, dense_in, dense_out
            )
        )
        for cells in sent
    ]
    out = None
    for chunk, cells in enumerate(returned):
        out = expand((chunk, CHUNKS) + shape + (breadth,), cells, input_field, expand_weight, out)
    return out


def solution(mesh):
    return jax.shard_map(
        per_device,
        mesh=mesh,
        in_specs=(P("lat", "lon", None), P(), P(), P(), P(), P(), P(), P(), P(), P()),
        out_specs=P("lat", "lon", None),
        check_vma=False,
    )
```

```python
import functools
import math

import jax
import jax.numpy as jnp
from jax import lax
from jax.experimental import pallas as pl
from jax.experimental.pallas import tpu as pltpu
from jax.sharding import PartitionSpec as P

WINDOW = 16
HEAD_WIDTH = 32
EPSILON = 1e-06
FLOOR = 0.75
CHUNKS = 2
F32 = jnp.float32
BF16 = jnp.bfloat16
LIMIT = 56 * 1024 * 1024


def dot(a, b):
    return jnp.dot(a, b, preferred_element_type=F32)


def padded(cells, sides, width):
    for axis, dim in sides:
        count = lax.axis_size(axis)
        ends = count - 1
        head = lax.slice_in_dim(cells, 0, width, axis=dim)
        tail = lax.slice_in_dim(cells, cells.shape[dim] - width, cells.shape[dim], axis=dim)
        cells = jnp.concatenate(
            [
                lax.ppermute(tail, axis, [(i, (i + 1) % count) for i in range(ends)]),
                cells,
                lax.ppermute(head, axis, [((i + 1) % count, i) for i in range(ends)]),
            ],
            axis=dim,
        )
    return cells


def pair_kernel(kernel_ref, paired):
    taps, _, c, o = kernel_ref.shape
    zero = jnp.zeros((c, o), BF16)
    for a in range(taps):
        for b in range(4):
            rows = slice((4 * a + b) * c, (4 * a + b + 1) * c)
            paired[rows, :o] = kernel_ref[a, b] if b < 3 else zero
            paired[rows, o:] = kernel_ref[a, b - 1] if b > 0 else zero


def encode_body(geo, place_ref, x_ref, k1_ref, k2_ref, mw_ref, out_ref, xs, fs, cs, w1_ref, w2_ref):
    (chunk, chunks, per_lat, per_lon, offset_lat, offset_lon, lat_total, lon_total, breadth, pairs) = geo
    band = pl.program_id(0)
    rows = 2 * offset_lat // chunks
    c = x_ref.shape[2]
    half = breadth // 2
    wide = breadth + 4

    @pl.when(band == 0)
    def _():
        pair_kernel(k1_ref, w1_ref)
        pair_kernel(k2_ref, w2_ref)
        xs[:, wide:, :] = jnp.zeros((rows + 4, xs.shape[1] - wide, c), F32)

    xs[:, :wide, :] = x_ref[...].astype(F32)
    quad = [
        xs[:, pl.ds(j, pairs, stride=2), :].astype(BF16) for j in range(4)
    ]
    lhs = jnp.concatenate(
        [q[a : a + rows + 2].reshape((rows + 2) * pairs, c) for a in range(3) for q in quad], axis=1
    )
    first = jax.nn.gelu(dot(lhs, w1_ref[...])).reshape(rows + 2, pairs, 2 * c)
    row = lax.broadcasted_iota(jnp.int32, first.shape, 0)
    pair = lax.broadcasted_iota(jnp.int32, first.shape, 1)
    lane = lax.broadcasted_iota(jnp.int32, first.shape, 2)
    lat_place = row + (place_ref[0] + band * 2 * offset_lat + chunk * rows - 1)
    lon_place = 2 * pair + (lane >= c).astype(jnp.int32) + (place_ref[1] - 1)
    inside = (lat_place >= 0) & (lat_place < lat_total) & (lon_place >= 0) & (lon_place < lon_total)
    fs[...] = jnp.where(inside, first, 0.0)
    near = fs[:, 0:half, :].astype(BF16)
    far = fs[:, pl.ds(1, half), :].astype(BF16)
    lhs = jnp.concatenate(
        [q[a : a + rows].reshape(rows * half, 2 * c) for a in range(3) for q in (near, far)], axis=1
    )
    second = jax.nn.gelu(dot(lhs, w2_ref[...])).astype(BF16)
    second = second.reshape(rows // 2, 2, half, 2 * c)
    patches = jnp.concatenate(
        [second[:, d].reshape(rows // 2 * half, 2 * c) for d in range(2)], axis=1
    )
    coarse = dot(patches, mw_ref[...]).astype(BF16).reshape(rows // 2, half, 4 * c)
    for u in range(rows // 2):
        cs[u, pl.ds(pl.multiple_of(band * half, half), half), :] = coarse[u]

    @pl.when(band == per_lat - 1)
    def _():
        count = per_lat * half
        tokens = per_lat * per_lon
        to = lax.broadcasted_iota(jnp.int32, (count, count), 0)
        of = lax.broadcasted_iota(jnp.int32, (count, count), 1)
        source = (to % tokens) * offset_lon + to // tokens
        move = (of == source).astype(F32).astype(BF16)
        for u in range(rows // 2):
            out_ref[u * count : (u + 1) * count, :] = dot(move, cs[u]).astype(BF16)


def encode(geo, place, widened, w1, w2, merge_weight):
    (chunk, chunks, per_lat, per_lon, offset_lat, offset_lon, lat_total, lon_total, breadth, pairs) = geo
    rows = 2 * offset_lat // chunks
    c = widened.shape[2]
    half = breadth // 2
    count = rows // 2 * per_lat * half
    full = lambda a: pl.BlockSpec(a.shape, lambda p: (0,) * a.ndim)
    flops = 2 * per_lat * ((rows + 2) * pairs + rows * half) * 12 * c * 2 * c
    return pl.pallas_call(
        functools.partial(encode_body, geo),
        grid=(per_lat,),
        in_specs=[
            pl.BlockSpec(memory_space=pltpu.SMEM),
            pl.BlockSpec(
                (pl.Element(rows + 4), pl.Element(breadth + 4), pl.Element(c)),
                lambda p: (p * 2 * offset_lat + chunk * rows, 0, 0),
            ),
            full(w1),
            full(w2),
            full(merge_weight),
        ],
        out_specs=pl.BlockSpec((count, 4 * c), lambda p: (0, 0)),
        out_shape=jax.ShapeDtypeStruct((count, 4 * c), BF16),
        scratch_shapes=[
            pltpu.VMEM((rows + 4, max(2 * pairs + 8, breadth + 8), c), F32),
            pltpu.VMEM((rows + 2, pairs, 2 * c), F32),
            pltpu.VMEM((rows // 2, per_lat * half, 4 * c), BF16),
            pltpu.VMEM((12 * c, 2 * c), BF16),
            pltpu.VMEM((12 * c, 2 * c), BF16),
        ],
        compiler_params=pltpu.CompilerParams(
            dimension_semantics=("arbitrary",), vmem_limit_bytes=LIMIT
        ),
        cost_estimate=pl.CostEstimate(flops=flops, bytes_accessed=4_000_000, transcendentals=0),
        name="encode",
    )(place, widened, w1, w2, merge_weight)


def layer_norm(stream, gain):
    center = stream - jnp.mean(stream, axis=-1, keepdims=True)
    spread = jnp.mean(center * center, axis=-1, keepdims=True)
    return center * lax.rsqrt(spread + EPSILON) * gain


def window_body(geo, x_ref, g_ref, ai_ref, ao_ref, di_ref, do_ref, out_ref):
    devices, windows, tokens = geo
    latent = x_ref.shape[-1]
    size = devices * tokens
    count = windows * size
    to = lax.broadcasted_iota(jnp.int32, (count, count), 0)
    of = lax.broadcasted_iota(jnp.int32, (count, count), 1)
    row = lax.broadcasted_iota(jnp.int32, (count, 1), 0)
    col = lax.broadcasted_iota(jnp.int32, (1, count), 1)

    def sorted_row(i):
        return (i // tokens % windows) * size + i // (tokens * windows) * tokens + i % tokens

    gather = (to == sorted_row(col)).astype(F32).astype(BF16)
    scatter = (of == sorted_row(row)).astype(F32).astype(BF16)
    coarse = dot(gather, x_ref[...].reshape(count, latent))
    gains = g_ref[...]
    normed = layer_norm(coarse, gains[0:1]).astype(BF16)
    head_row = lax.broadcasted_iota(jnp.int32, (latent, latent), 0) // HEAD_WIDTH
    head_col = lax.broadcasted_iota(jnp.int32, (latent, latent), 1) // HEAD_WIDTH
    spread = jnp.where(head_row == head_col, 1.0 / HEAD_WIDTH, 0.0).astype(BF16)

    def head_norm(stream, gain):
        square = dot((stream * stream).astype(BF16), spread)
        return (stream * gain * lax.rsqrt(jnp.maximum(square, FLOOR))).astype(BF16)

    queries = head_norm(dot(normed, ai_ref[:, :latent]), gains[1:2])
    key_rows = head_norm(dot(normed, ai_ref[:, latent : 2 * latent]), gains[2:3])
    values = dot(normed, ai_ref[:, 2 * latent :]).astype(BF16)
    group = 128
    heads = group // HEAD_WIDTH
    lane = lax.broadcasted_iota(jnp.int32, (size, group), 1) // HEAD_WIDTH
    marks = [(lane == h).astype(F32).astype(BF16) for h in range(heads)]
    scale = HEAD_WIDTH ** (-0.5) * math.log2(math.e)
    parts = []
    for win in range(windows):
        span = slice(win * size, (win + 1) * size)
        row_parts = []
        for at in range(0, latent, group):
            q = queries[span, at : at + group]
            k = key_rows[span, at : at + group]
            v = values[span, at : at + group]
            expons = []
            stacked = []
            for h in range(heads):
                scores = lax.dot_general(
                    q * marks[h], k, (((1,), (1,)), ((), ())), preferred_element_type=F32
                )
                expons.append(jnp.exp2(scores * scale).astype(BF16))
                stacked.append(jnp.concatenate([v * marks[h], marks[h]], axis=1))
            both = dot(jnp.concatenate(expons, axis=1), jnp.concatenate(stacked, axis=0))
            row_parts.append((both[:, :group] / both[:, group:]).astype(BF16))
        parts.append(jnp.concatenate(row_parts, axis=1))
    attended = jnp.concatenate(parts, axis=0)
    mixed = (coarse + dot(attended, ao_ref[...])).astype(BF16)
    normed_two = layer_norm(mixed.astype(F32), gains[3:4]).astype(BF16)
    total = mixed.astype(F32)
    width = di_ref.shape[1]
    step = min(512, width)
    for at in range(0, width, step):
        inner = jax.nn.gelu(dot(normed_two, di_ref[:, at : at + step])).astype(BF16)
        total = total + dot(inner, do_ref[at : at + step, :])
    out_ref[...] = dot(scatter, total.astype(BF16)).astype(BF16).reshape(out_ref.shape)


def windows_of(geo, cells, gains, attention_in, attention_out, dense_in, dense_out):
    devices, windows, tokens = geo
    count, latent = cells.shape
    fits = [n for n in range(1, windows) if windows % n == 0 and n * tokens % 16 == 0]
    full = lambda a: pl.BlockSpec(a.shape, lambda i: (0,) * a.ndim)
    if fits:
        block = fits[0]
        cells = cells.reshape(devices, windows * tokens, latent)
        place = pl.BlockSpec((devices, block * tokens, latent), lambda i: (0, i, 0))
    else:
        block = windows
        place = full(cells)
    weights = (gains, attention_in, attention_out, dense_in, dense_out)
    flops = 2 * count * latent * (4 * latent + 2 * dense_in.shape[1] + 4 * count)
    made = pl.pallas_call(
        functools.partial(window_body, (devices, block, tokens)),
        grid=(windows // block,),
        out_shape=jax.ShapeDtypeStruct(cells.shape, BF16),
        in_specs=[place] + [full(a) for a in weights],
        out_specs=place,
        compiler_params=pltpu.CompilerParams(
            dimension_semantics=("arbitrary",), vmem_limit_bytes=LIMIT
        ),
        cost_estimate=pl.CostEstimate(flops=flops, bytes_accessed=8_000_000, transcendentals=0),
        name="windows",
    )(cells, *weights)
    return made.reshape(count, latent)


def expand_body(geo, aliased, ret_ref, x_ref, ew_ref, *rest):
    (chunk, chunks, per_lat, per_lon, offset_lat, offset_lon, breadth) = geo
    out_ref, os = rest[-2:]
    band = pl.program_id(0)
    lines = offset_lat // chunks
    c = x_ref.shape[2]
    half = breadth // 2
    tokens = per_lat * per_lon
    count = per_lat * half
    to = lax.broadcasted_iota(jnp.int32, (half, count), 0)
    of = lax.broadcasted_iota(jnp.int32, (half, count), 1)
    source = (to % offset_lon) * tokens + band * per_lon + to // offset_lon
    move = (of == source).astype(F32).astype(BF16)
    cells = jnp.concatenate(
        [dot(move, ret_ref[u * count : (u + 1) * count, :]).astype(BF16) for u in range(lines)], axis=0
    )
    made = dot(cells, ew_ref[...])
    for u in range(lines):
        for d in range(4):
            os[2 * u + d // 2, pl.ds(d % 2, half, stride=2), :] = made[
                u * half : (u + 1) * half, d * c : (d + 1) * c
            ]
    out_ref[...] = (os[...] + x_ref[...].astype(F32)).astype(BF16)


def expand(geo, returned, field, expand_weight, buffer):
    (chunk, chunks, per_lat, per_lon, offset_lat, offset_lon, breadth) = geo
    rows = 2 * offset_lat // chunks
    c = field.shape[2]
    aliased = buffer is not None
    place = pl.BlockSpec((rows, breadth, c), lambda p: (p * chunks + chunk, 0, 0))
    in_specs = [
        pl.BlockSpec(returned.shape, lambda p: (0, 0)),
        place,
        pl.BlockSpec(expand_weight.shape, lambda p: (0, 0)),
    ]
    args = [returned, field, expand_weight]
    if aliased:
        in_specs.append(pl.BlockSpec(memory_space=pl.ANY))
        args.append(buffer)
    return pl.pallas_call(
        functools.partial(expand_body, geo, aliased),
        grid=(per_lat,),
        in_specs=in_specs,
        out_specs=place,
        out_shape=jax.ShapeDtypeStruct(field.shape, BF16),
        scratch_shapes=[pltpu.VMEM((rows, breadth, c), F32)],
        input_output_aliases={3: 0} if aliased else {},
        compiler_params=pltpu.CompilerParams(
            dimension_semantics=("arbitrary",), vmem_limit_bytes=LIMIT
        ),
        cost_estimate=pl.CostEstimate(
            flops=2 * returned.size * 4 * c, bytes_accessed=3_000_000, transcendentals=0
        ),
        name="expand",
    )(*args)


def per_device(
    input_field,
    conv_one,
    conv_two,
    merge_weight,
    norm_gains,
    attention_in,
    attention_out,
    dense_in,
    dense_out,
    expand_weight,
):
    height, breadth, _ = input_field.shape
    latent = merge_weight.shape[1]
    lat_count = lax.axis_size("lat")
    lon_count = lax.axis_size("lon")
    per_lat = WINDOW // lat_count
    per_lon = WINDOW // lon_count
    offset_lat = height // (2 * per_lat)
    offset_lon = breadth // (2 * per_lon)
    tokens = per_lat * per_lon
    devices = lat_count * lon_count
    windows = offset_lat * offset_lon // devices // CHUNKS
    pairs = -(-(breadth // 2 + 1) // 16) * 16
    place = jnp.stack([lax.axis_index("lat") * height, lax.axis_index("lon") * breadth]).astype(jnp.int32)
    widened = padded(input_field, (("lat", 0), ("lon", 1)), 2)

    def exchange(cells):
        moved = lax.all_to_all(
            cells.reshape(devices, windows * tokens, latent),
            ("lat", "lon"),
            split_axis=0,
            concat_axis=0,
            tiled=True,
        )
        return moved.reshape(cells.shape)

    shape = (per_lat, per_lon, offset_lat, offset_lon)
    sent = [
        exchange(
            encode(
                (chunk, CHUNKS) + shape + (height * lat_count, breadth * lon_count, breadth, pairs),
                place,
                widened,
                conv_one,
                conv_two,
                merge_weight,
            )
        )
        for chunk in range(CHUNKS)
    ]
    returned = [
        exchange(
            windows_of(
                (devices, windows, tokens), cells, norm_gains, attention_in, attention_out, dense_in, dense_out
            )
        )
        for cells in sent
    ]
    out = None
    for chunk, cells in enumerate(returned):
        out = expand((chunk, CHUNKS) + shape + (breadth,), cells, input_field, expand_weight, out)
    return out


def solution(mesh):
    return jax.shard_map(
        per_device,
        mesh=mesh,
        in_specs=(P("lat", "lon", None), P(), P(), P(), P(), P(), P(), P(), P(), P()),
        out_specs=P("lat", "lon", None),
        check_vma=False,
    )
```
